8 devices in a mesh: dp: 2 (over y, z), tp: 4 (over x, core).
Axes of the slice: x: 2, y: 2, z: 1, core: 2. Of those that a mesh axis runs over, the one named last changes fastest.
Arguments:
- x: bfloat16 [8, 512, 12288], P('dp'), parts along dimension 0
- gain_a: bfloat16 [12288], replicated
- wq: bfloat16 [12288, 12288], P(None, 'tp')
- wk: bfloat16 [12288, 1024], P(None, 'tp')
- wv: bfloat16 [12288, 1024], P(None, 'tp')
- wo: bfloat16 [12288, 12288], P('tp')
- gain_m: bfloat16 [12288], replicated
- w_gate: bfloat16 [12288, 28672], P(None, 'tp')
- w_up: bfloat16 [12288, 28672], P(None, 'tp')
- w_down: bfloat16 [28672, 12288], P('tp')
Outputs:
- output: bfloat16 [8, 512, 12288], P('dp'), parts along dimension 0
There are 2 independent parts. The reference program is written for one: setup_inputs(seed, part) draws one part's arguments, and reference() takes and returns one part's arrays. A program takes and returns all parts, laid end to end along the dimension named above; an argument that names none is the same for every part.
All inputs are finite; a program needn't handle non-finite values.
Results may differ from the reference program's by a relative error of at most 0.017.
Values are sent between devices in bfloat16 or wider.
A program may use at most 2.5 GiB of HBM per device.

```python
import jax
import jax.numpy as jnp
from jax import lax

SEQUENCES = 4
TOKENS = 512
D = 12288
HEADS = 96
KV_HEADS = 8
HEAD = 128
FF = 28672
THETA = 10000


def setup_inputs(seed: int = 0, part: int = 0) -> dict:
    kx, ka, km, kq, kk, kv, ko, kg, ku, kd = jax.random.split(jax.random.key(seed), 10)

    def weights(key, rows, columns):
        return jax.random.normal(key, (rows, columns), jnp.float32) * rows**-0.5

    drawn = {
        "x": jax.random.normal(jax.random.fold_in(kx, part), (SEQUENCES, TOKENS, D), jnp.float32),
        "gain_a": 1 + 0.1 * jax.random.normal(ka, (D,), jnp.float32),
        "wq": 2 * weights(kq, D, HEADS * HEAD),
        "wk": 2 * weights(kk, D, KV_HEADS * HEAD),
        "wv": 4 * weights(kv, D, KV_HEADS * HEAD),
        "wo": weights(ko, HEADS * HEAD, D),
        "gain_m": 1 + 0.1 * jax.random.normal(km, (D,), jnp.float32),
        "w_gate": weights(kg, D, FF),
        "w_up": weights(ku, D, FF),
        "w_down": 3 * weights(kd, FF, D),
    }
    return {k: v.astype(jnp.bfloat16) for k, v in drawn.items()}


def normed(x, gain):
    wide = x.astype(jnp.float32)
    scale = lax.rsqrt(jnp.mean(wide * wide, -1, keepdims=True) + 1e-6)
    return (wide * scale * gain.astype(jnp.float32)).astype(jnp.bfloat16)


def turned(t, place, theta):
    half = t.shape[-1] // 2
    angle = place.astype(jnp.float32)[:, None] * theta ** (-jnp.arange(half, dtype=jnp.float32) / half)
    cos, sin = jnp.cos(angle)[:, None], jnp.sin(angle)[:, None]
    a, b = t[..., :half].astype(jnp.float32), t[..., half:].astype(jnp.float32)
    return jnp.concatenate([a * cos - b * sin, b * cos + a * sin], -1).astype(jnp.bfloat16)


def matmul(a, w):
    return jnp.dot(a, w, preferred_element_type=jnp.float32).astype(jnp.bfloat16)


def einsum(form, a, b):
    return jnp.einsum(form, a.astype(jnp.float32), b.astype(jnp.float32))


def attention(q, k, v):
    scores = einsum("tgsd,ugd->gstu", q, k) * q.shape[-1] ** -0.5
    token = jnp.arange(q.shape[0])
    scores = jnp.where(token[:, None] >= token, scores, -jnp.inf)
    weights = jax.nn.softmax(scores, -1).astype(jnp.bfloat16)
    return einsum("gstu,ugd->tgsd", weights, v).astype(jnp.bfloat16)


def one(x, gain_a, wq, wk, wv, wo, gain_m, w_gate, w_up, w_down):
    rows = x.shape[0]
    a, place = normed(x, gain_a), jnp.arange(rows)
    k = turned(matmul(a, wk).reshape(rows, -1, HEAD), place, THETA)
    q = turned(matmul(a, wq).reshape(rows, -1, HEAD), place, THETA).reshape(rows, k.shape[1], -1, HEAD)
    v = matmul(a, wv).reshape(rows, -1, HEAD)
    seen = attention(q, k, v).reshape(rows, -1)
    h = (x.astype(jnp.float32) + jnp.dot(seen, wo, preferred_element_type=jnp.float32)).astype(jnp.bfloat16)
    b = normed(h, gain_m)
    gate = jnp.dot(b, w_gate, preferred_element_type=jnp.float32)
    up = jnp.dot(b, w_up, preferred_element_type=jnp.float32)
    hidden = (jax.nn.silu(gate) * up).astype(jnp.bfloat16)
    return (h.astype(jnp.float32) + jnp.dot(hidden, w_down, preferred_element_type=jnp.float32)).astype(jnp.bfloat16)


def reference(x, gain_a, wq, wk, wv, wo, gain_m, w_gate, w_up, w_down):
    return lax.map(lambda sequence: one(sequence, gain_a, wq, wk, wv, wo, gain_m, w_gate, w_up, w_down), x)
```

```python
import functools

import jax
import jax.numpy as jnp
from jax import lax
from jax.experimental import pallas as pl
from jax.experimental.pallas import tpu as pltpu
from jax.sharding import PartitionSpec as P

HEAD = 128
THETA = 10000
HIDDEN = -2e30
LOG2E = 1.4426950408889634
VMEM = 56 * 2**20
MATE = [(0, 1), (1, 0), (2, 3), (3, 2)]
ACROSS = [(0, 2), (2, 0), (1, 3), (3, 1)]
PIECES_A = (2, 2)
PIECES_M = (1, 4)


def _dot(a, b, ca, cb):
    return lax.dot_general(a, b, (((ca,), (cb,)), ((), ())), preferred_element_type=jnp.float32)


def _attention(order_ref, q_ref, k_ref, v_ref, cos_ref, sin_ref, o_ref, *, scale):
    rows, dtype = k_ref.shape[0], k_ref.dtype
    half = rows // 2
    e = scale * LOG2E
    cos, sin = cos_ref[...], sin_ref[...]

    def turn(t):
        t = t.astype(jnp.float32)
        return (t * cos + pltpu.roll(t, HEAD // 2, 1) * sin).astype(dtype)

    k = turn(k_ref[...])
    values = jnp.concatenate([v_ref[...].T, jnp.ones((8, rows), dtype)], axis=0)
    ok = lax.broadcasted_iota(jnp.int32, (half, half), 1) >= lax.broadcasted_iota(jnp.int32, (half, half), 0)
    heads = q_ref.shape[1] // HEAD
    together = 4
    for base in range(0, heads, together):
        group = range(base, min(base + together, heads))
        qs = [turn(q_ref[:, h * HEAD : (h + 1) * HEAD]) for h in group]
        upper = [_dot(k[:half], q, 1, 1) for q in qs]
        lower = [_dot(k[half:], q[half:], 1, 1) for q in qs]
        early, late = [], []
        for u, w in zip(upper, lower):
            a, b, c = jnp.where(ok, u[:, :half], HIDDEN), u[:, half:], jnp.where(ok, w, HIDDEN)
            top = a.max(axis=0, keepdims=True)
            early.append(jnp.exp2((a - top) * e).astype(dtype))
            top = jnp.maximum(b.max(axis=0, keepdims=True), c.max(axis=0, keepdims=True))
            late.append(jnp.concatenate([jnp.exp2((b - top) * e).astype(dtype), jnp.exp2((c - top) * e).astype(dtype)], axis=0))
        for h, p0, p1 in zip(group, early, late):
            for at, mix in ((0, _dot(values[:, :half], p0, 1, 0)), (half, _dot(values, p1, 1, 0))):
                out = mix[:HEAD] * (1 / mix[HEAD : HEAD + 1])
                o_ref[at : at + half, h * HEAD : (h + 1) * HEAD] = out.T.astype(o_ref.dtype)


def attention(q, k, v, order, cos, sin, rows):
    n, kv = q.shape[0] // rows, k.shape[1] // HEAD
    width = q.shape[1] // kv
    small = pl.BlockSpec((rows, HEAD), lambda s, h, order_ref: (order_ref[s], h))
    table = pl.BlockSpec((rows, HEAD), lambda s, h, order_ref: (0, 0))
    pairs = n * (q.shape[1] // HEAD) * rows * rows
    return pl.pallas_call(
        functools.partial(_attention, scale=HEAD**-0.5),
        grid_spec=pltpu.PrefetchScalarGridSpec(
            num_scalar_prefetch=1,
            grid=(n, kv),
            in_specs=[pl.BlockSpec((rows, width), lambda s, h, order_ref: (order_ref[s], h)), small, small, table, table],
            out_specs=pl.BlockSpec((rows, width), lambda s, h, order_ref: (s, h)),
        ),
        out_shape=jax.ShapeDtypeStruct(q.shape, q.dtype),
        compiler_params=pltpu.CompilerParams(dimension_semantics=("arbitrary", "arbitrary"), vmem_limit_bytes=VMEM),
        cost_estimate=pl.CostEstimate(flops=4 * pairs * HEAD, transcendentals=pairs, bytes_accessed=4 * q.size + 4 * k.size),
    )(order, q, k, v, cos, sin)


WIDE = 512
TALL = 64


def _scaled(from_ref, total, gain_ref, to_ref):
    d = from_ref.shape[1]
    scale = lax.rsqrt(total.sum(axis=1, keepdims=True) * (1 / d) + 1e-6)

    def scaled(n, _):
        cols = pl.ds(pl.multiple_of(n * WIDE, WIDE), WIDE)
        gain = gain_ref[:, cols].astype(jnp.float32)
        to_ref[:, cols] = (from_ref[:, cols].astype(jnp.float32) * scale * gain).astype(to_ref.dtype)

    lax.fori_loop(0, d // WIDE, scaled, None, unroll=4)


def _norm(x_ref, gain_ref, o_ref):
    def square(n, total):
        wide = x_ref[0, :, pl.ds(pl.multiple_of(n * WIDE, WIDE), WIDE)].astype(jnp.float32)
        return total + wide * wide

    total = lax.fori_loop(0, x_ref.shape[2] // WIDE, square, jnp.zeros((x_ref.shape[1], WIDE), jnp.float32), unroll=4)
    _scaled(x_ref.at[0], total, gain_ref, o_ref)


def norm(x, gain, first, count):
    _, rows, d = x.shape
    per = rows // TALL
    return pl.pallas_call(
        _norm,
        grid=(count * per,),
        in_specs=[pl.BlockSpec((1, TALL, d), lambda i: (first + i // per, i % per, 0)), pl.BlockSpec((1, d), lambda i: (0, 0))],
        out_specs=pl.BlockSpec((TALL, d), lambda i: (i, 0)),
        out_shape=jax.ShapeDtypeStruct((count * rows, d), x.dtype),
        compiler_params=pltpu.CompilerParams(dimension_semantics=("arbitrary",), vmem_limit_bytes=VMEM),
        cost_estimate=pl.CostEstimate(flops=100 * count * rows * d, transcendentals=0, bytes_accessed=4 * count * rows * d),
    )(x, gain.reshape(1, d))


def _join(mine_ref, x_ref, gain_ref, *refs, pieces):
    here, there, (h_ref, b_ref) = refs[:pieces], refs[pieces : 2 * pieces], refs[2 * pieces :]
    total = jnp.zeros((x_ref.shape[1], WIDE), jnp.float32)
    for p, (s_ref, t_ref) in enumerate(zip(here, there)):
        width = s_ref.shape[1]

        def add(n, total, p=p, s_ref=s_ref, t_ref=t_ref, width=width):
            cols = pl.ds(pl.multiple_of(n * WIDE, WIDE), WIDE)
            at = pl.ds(pl.multiple_of(p * width + n * WIDE, WIDE), WIDE)
            both = s_ref[:, cols].astype(jnp.float32) + t_ref[:, cols].astype(jnp.float32)
            h = (x_ref[0, :, at].astype(jnp.float32) + both).astype(h_ref.dtype)
            h_ref[:, at] = h
            wide = h.astype(jnp.float32)
            return total + wide * wide

        total = lax.fori_loop(0, width // WIDE, add, total, unroll=4)
    _scaled(h_ref, total, gain_ref, b_ref)


def join(x, gain, mine, here, there):
    _, rows, d = x.shape
    row = lambda i, mine_ref: (i, 0)
    terms = [pl.BlockSpec((TALL, t.shape[1]), row) for t in (*here, *there)]
    whole = jax.ShapeDtypeStruct((rows, d), x.dtype)
    return pl.pallas_call(
        functools.partial(_join, pieces=len(here)),
        grid_spec=pltpu.PrefetchScalarGridSpec(
            num_scalar_prefetch=1,
            grid=(rows // TALL,),
            in_specs=[pl.BlockSpec((1, TALL, d), lambda i, mine_ref: (mine_ref[0], i, 0)),
                      pl.BlockSpec((1, d), lambda i, mine_ref: (0, 0)), *terms],
            out_specs=[pl.BlockSpec((TALL, d), row)] * 2,
        ),
        out_shape=[whole, whole],
        compiler_params=pltpu.CompilerParams(dimension_semantics=("arbitrary",), vmem_limit_bytes=VMEM),
        cost_estimate=pl.CostEstimate(flops=200 * rows * d, transcendentals=0, bytes_accessed=10 * rows * d),
    )(mine.reshape(1), x, gain.reshape(1, d), *here, *there)


def dot(a, w):
    return jnp.dot(a, w, preferred_element_type=jnp.float32)


def matmul(a, w):
    return dot(a, w).astype(jnp.bfloat16)


def _nothing(out_ref):
    pass


def unwritten(shape, dtype):
    return pl.pallas_call(_nothing, out_specs=pl.BlockSpec(memory_space=pl.ANY), out_shape=jax.ShapeDtypeStruct(shape, dtype))()


def summed(theirs, mine, w, pieces):
    width = w.shape[1] // pieces
    parts = [w[:, n * width : (n + 1) * width] for n in range(pieces)]
    given, here, there = [], [], []
    for part in parts:
        term = matmul(theirs, part)
        given.append(lax.ppermute(term, "tp", MATE))
    for part, term in zip(parts, given):
        here.append((dot(mine, part) + term.astype(jnp.float32)).astype(jnp.bfloat16))
        there.append(lax.ppermute(here[-1], "tp", ACROSS))
    return here, there


def joined(base, here, there):
    return (base.astype(jnp.float32) + (here.astype(jnp.float32) + there.astype(jnp.float32))).astype(jnp.bfloat16)


def solution(mesh):
    def step(x, gain_a, wq, wk, wv, wo, gain_m, w_gate, w_up, w_down):
        batch, rows, d = x.shape
        core = lax.rem(lax.axis_index("tp"), 2)
        half = HEAD // 2
        angle = jnp.arange(rows).astype(jnp.float32)[:, None] * THETA ** (-jnp.arange(half, dtype=jnp.float32) / half)
        cos, sin = jnp.cos(angle), jnp.sin(angle)
        cos, sin = jnp.concatenate([cos, cos], 1), jnp.concatenate([-sin, sin], 1)
        order = jnp.stack([1 - core, core]).astype(jnp.int32)
        pairs = range(batch // 2)

        sums = []
        for p in pairs:
            a = norm(x, gain_a, 2 * p, 2)
            v, k, q = matmul(a, wv), matmul(a, wk), matmul(a, wq)
            seen = attention(q, k, v, order, cos, sin, rows)
            sums.append(summed(seen[:rows], seen[rows:], wo, PIECES_A[p]))

        def gated(b):
            up = lax.optimization_barrier(dot(b, w_up))
            return (jax.nn.silu(dot(b, w_gate)) * up).astype(jnp.bfloat16)

        y = unwritten(x.shape, x.dtype)
        for p in pairs:
            mine = (2 * p + core).astype(jnp.int32)
            h, b = join(x, gain_m, mine, *sums[p])
            b_mate = lax.ppermute(b, "tp", MATE)
            hidden = gated(b)
            hidden_mate = gated(b_mate)
            here, there = summed(hidden_mate, hidden, w_down, PIECES_M[p])
            width = d // len(here)
            for n, (s, t) in enumerate(zip(here, there)):
                own = joined(h[:, n * width : (n + 1) * width], s, t)
                other = lax.ppermute(own, "tp", MATE)
                y = lax.dynamic_update_slice(y, own[None], (mine, 0, n * width))
                y = lax.dynamic_update_slice(y, other[None], (2 * p + 1 - core, 0, n * width))
        return y

    tokens, whole, columns, rows_of = P("dp", None, None), P(None), P(None, "tp"), P("tp", None)
    return jax.shard_map(
        step,
        mesh=mesh,
        in_specs=(tokens, whole, columns, columns, columns, rows_of, whole, columns, columns, rows_of),
        out_specs=tokens,
        check_vma=False,
    )
```

```python
import functools

import jax
import jax.numpy as jnp
from jax import lax
from jax.experimental import pallas as pl
from jax.experimental.pallas import tpu as pltpu
from jax.sharding import PartitionSpec as P

HEAD = 128
THETA = 10000
HIDDEN = -2e30
LOG2E = 1.4426950408889634
VMEM = 56 * 2**20
MATE = [(0, 1), (1, 0), (2, 3), (3, 2)]
ACROSS = [(0, 2), (2, 0), (1, 3), (3, 1)]
PIECES_A = (2, 2)
PIECES_M = (1, 4)


def _dot(a, b, ca, cb):
    return lax.dot_general(a, b, (((ca,), (cb,)), ((), ())), preferred_element_type=jnp.float32)


def _attention(order_ref, q_ref, k_ref, v_ref, cos_ref, sin_ref, o_ref, *, scale):
    rows, dtype = k_ref.shape[0], k_ref.dtype
    half = rows // 2
    e = scale * LOG2E
    cos, sin = cos_ref[...], sin_ref[...]

    def turn(t):
        t = t.astype(jnp.float32)
        return (t * cos + pltpu.roll(t, HEAD // 2, 1) * sin).astype(dtype)

    k = turn(k_ref[...])
    values = jnp.concatenate([v_ref[...].T, jnp.ones((8, rows), dtype)], axis=0)
    ok = lax.broadcasted_iota(jnp.int32, (half, half), 1) >= lax.broadcasted_iota(jnp.int32, (half, half), 0)
    heads = q_ref.shape[1] // HEAD
    together = 4
    for base in range(0, heads, together):
        group = range(base, min(base + together, heads))
        qs = [turn(q_ref[:, h * HEAD : (h + 1) * HEAD]) for h in group]
        upper = [_dot(k[:half], q, 1, 1) for q in qs]
        lower = [_dot(k[half:], q[half:], 1, 1) for q in qs]
        early, late = [], []
        for u, w in zip(upper, lower):
            a, b, c = jnp.where(ok, u[:, :half], HIDDEN), u[:, half:], jnp.where(ok, w, HIDDEN)
            top = a.max(axis=0, keepdims=True)
            early.append(jnp.exp2((a - top) * e).astype(dtype))
            top = jnp.maximum(b.max(axis=0, keepdims=True), c.max(axis=0, keepdims=True))
            late.append(jnp.concatenate([jnp.exp2((b - top) * e).astype(dtype), jnp.exp2((c - top) * e).astype(dtype)], axis=0))
        for h, p0, p1 in zip(group, early, late):
            for at, mix in ((0, _dot(values[:, :half], p0, 1, 0)), (half, _dot(values, p1, 1, 0))):
                out = mix[:HEAD] * (1 / mix[HEAD : HEAD + 1])
                o_ref[at : at + half, h * HEAD : (h + 1) * HEAD] = out.T.astype(o_ref.dtype)


def attention(q, k, v, order, cos, sin, rows):
    n, kv = q.shape[0] // rows, k.shape[1] // HEAD
    width = q.shape[1] // kv
    small = pl.BlockSpec((rows, HEAD), lambda s, h, order_ref: (order_ref[s], h))
    table = pl.BlockSpec((rows, HEAD), lambda s, h, order_ref: (0, 0))
    pairs = n * (q.shape[1] // HEAD) * rows * rows
    return pl.pallas_call(
        functools.partial(_attention, scale=HEAD**-0.5),
        grid_spec=pltpu.PrefetchScalarGridSpec(
            num_scalar_prefetch=1,
            grid=(n, kv),
            in_specs=[pl.BlockSpec((rows, width), lambda s, h, order_ref: (order_ref[s], h)), small, small, table, table],
            out_specs=pl.BlockSpec((rows, width), lambda s, h, order_ref: (s, h)),
        ),
        out_shape=jax.ShapeDtypeStruct(q.shape, q.dtype),
        compiler_params=pltpu.CompilerParams(dimension_semantics=("arbitrary", "arbitrary"), vmem_limit_bytes=VMEM),
        cost_estimate=pl.CostEstimate(flops=4 * pairs * HEAD, transcendentals=pairs, bytes_accessed=4 * q.size + 4 * k.size),
    )(order, q, k, v, cos, sin)


WIDE = 256
TALL = 64


def _scaled(from_ref, total, gain_ref, to_ref):
    d = from_ref.shape[1]
    scale = lax.rsqrt(total.sum(axis=1, keepdims=True) * (1 / d) + 1e-6)

    def scaled(n, _):
        cols = pl.ds(pl.multiple_of(n * WIDE, WIDE), WIDE)
        gain = gain_ref[:, cols].astype(jnp.float32)
        to_ref[:, cols] = (from_ref[:, cols].astype(jnp.float32) * scale * gain).astype(to_ref.dtype)

    lax.fori_loop(0, d // WIDE, scaled, None, unroll=4)


def _norm(x_ref, gain_ref, o_ref):
    def square(n, total):
        wide = x_ref[0, :, pl.ds(pl.multiple_of(n * WIDE, WIDE), WIDE)].astype(jnp.float32)
        return total + wide * wide

    total = lax.fori_loop(0, x_ref.shape[2] // WIDE, square, jnp.zeros((x_ref.shape[1], WIDE), jnp.float32), unroll=4)
    _scaled(x_ref.at[0], total, gain_ref, o_ref)


def norm(x, gain, first, count):
    _, rows, d = x.shape
    tall = 2 * TALL
    per = rows // tall
    return pl.pallas_call(
        _norm,
        grid=(count * per,),
        in_specs=[pl.BlockSpec((1, tall, d), lambda i: (first + i // per, i % per, 0)), pl.BlockSpec((1, d), lambda i: (0, 0))],
        out_specs=pl.BlockSpec((tall, d), lambda i: (i, 0)),
        out_shape=jax.ShapeDtypeStruct((count * rows, d), x.dtype),
        compiler_params=pltpu.CompilerParams(dimension_semantics=("arbitrary",), vmem_limit_bytes=VMEM),
        cost_estimate=pl.CostEstimate(flops=100 * count * rows * d, transcendentals=0, bytes_accessed=4 * count * rows * d),
    )(x, gain.reshape(1, d))


def _join(x_ref, gain_ref, *refs, pieces):
    here, there = refs[:pieces], refs[pieces : 2 * pieces]
    h_ref, all_ref, buf, put_sem, send_sem, recv_sem = refs[2 * pieces :]
    step, steps = pl.program_id(0), pl.num_programs(0)
    slot = lax.rem(step, 2)
    tall = buf.shape[1]
    rows = all_ref.shape[0] // 2
    me = lax.axis_index("tp")
    mate = {"tp": me + 1 - 2 * lax.rem(me, 2)}

    def kept(at, slot):
        place = pl.ds(pl.multiple_of(rows + at * tall, tall), tall)
        return pltpu.make_async_copy(buf.at[slot], all_ref.at[place], put_sem.at[slot])

    def sent(at, slot):
        place = pl.ds(pl.multiple_of(at * tall, tall), tall)
        return pltpu.make_async_remote_copy(src_ref=buf.at[slot], dst_ref=all_ref.at[place], send_sem=send_sem.at[slot], recv_sem=recv_sem,
                                            device_id=mate, device_id_type=pl.DeviceIdType.MESH)

    @pl.when(step == 0)
    def _():
        barrier = pltpu.get_barrier_semaphore()
        pl.semaphore_signal(barrier, inc=1, device_id=mate, device_id_type=pl.DeviceIdType.MESH)
        pl.semaphore_wait(barrier, 1)

    @pl.when(step >= 2)
    def _():
        kept(step - 2, slot).wait()
        sent(step - 2, slot).wait_send()

    total = jnp.zeros((tall, WIDE), jnp.float32)
    for p, (s_ref, t_ref) in enumerate(zip(here, there)):
        width = s_ref.shape[1]

        def add(n, total, p=p, s_ref=s_ref, t_ref=t_ref, width=width):
            cols = pl.ds(pl.multiple_of(n * WIDE, WIDE), WIDE)
            at = pl.ds(pl.multiple_of(p * width + n * WIDE, WIDE), WIDE)
            both = s_ref[:, cols].astype(jnp.float32) + t_ref[:, cols].astype(jnp.float32)
            h = (x_ref[0, :, at].astype(jnp.float32) + both).astype(h_ref.dtype)
            h_ref[:, at] = h
            wide = h.astype(jnp.float32)
            return total + wide * wide

        total = lax.fori_loop(0, width // WIDE, add, total, unroll=4)
    _scaled(h_ref, total, gain_ref, buf.at[slot])
    kept(step, slot).start()
    sent(step, slot).start()

    @pl.when(step == steps - 1)
    def _():
        for back in (1, 0):
            kept(step - back, lax.rem(step - back, 2)).wait()
            sent(step - back, lax.rem(step - back, 2)).wait_send()
        half = all_ref.at[pl.ds(0, rows)]
        pltpu.make_async_copy(half, half, recv_sem).wait()


def join(x, gain, first, here, there):
    _, rows, d = x.shape
    row = lambda i: (i, 0)
    terms = [pl.BlockSpec((TALL, t.shape[1]), row) for t in (*here, *there)]
    return pl.pallas_call(
        functools.partial(_join, pieces=len(here)),
        grid=(rows // TALL,),
        in_specs=[pl.BlockSpec((1, TALL, d), lambda i: (first + lax.rem(lax.axis_index("tp"), 2), i, 0)),
                  pl.BlockSpec((1, d), lambda i: (0, 0)), *terms],
        out_specs=[pl.BlockSpec((TALL, d), row), pl.BlockSpec(memory_space=pl.ANY)],
        out_shape=[jax.ShapeDtypeStruct((rows, d), x.dtype), jax.ShapeDtypeStruct((2 * rows, d), x.dtype)],
        scratch_shapes=[pltpu.VMEM((2, TALL, d), x.dtype), pltpu.SemaphoreType.DMA((2,)), pltpu.SemaphoreType.DMA((2,)),
                        pltpu.SemaphoreType.DMA],
        compiler_params=pltpu.CompilerParams(dimension_semantics=("arbitrary",), vmem_limit_bytes=VMEM, collective_id=first,
                                             has_side_effects=True),
        cost_estimate=pl.CostEstimate(flops=200 * rows * d, transcendentals=0, bytes_accessed=12 * rows * d),
    )(x, gain.reshape(1, d), *here, *there)


def dot(a, w):
    return jnp.dot(a, w, preferred_element_type=jnp.float32)


def matmul(a, w):
    return dot(a, w).astype(jnp.bfloat16)


def _nothing(out_ref):
    pass


def unwritten(shape, dtype):
    return pl.pallas_call(_nothing, out_specs=pl.BlockSpec(memory_space=pl.ANY), out_shape=jax.ShapeDtypeStruct(shape, dtype))()


def summed(theirs, mine, w, pieces):
    width = w.shape[1] // pieces
    parts = [w[:, n * width : (n + 1) * width] for n in range(pieces)]
    given, here, there = [], [], []
    for part in parts:
        term = matmul(theirs, part)
        given.append(lax.ppermute(term, "tp", MATE))
    for part, term in zip(parts, given):
        here.append((dot(mine, part) + term.astype(jnp.float32)).astype(jnp.bfloat16))
        there.append(lax.ppermute(here[-1], "tp", ACROSS))
    return here, there


def joined(base, here, there):
    return (base.astype(jnp.float32) + (here.astype(jnp.float32) + there.astype(jnp.float32))).astype(jnp.bfloat16)


def solution(mesh):
    def step(x, gain_a, wq, wk, wv, wo, gain_m, w_gate, w_up, w_down):
        batch, rows, d = x.shape
        core = lax.rem(lax.axis_index("tp"), 2)
        half = HEAD // 2
        angle = jnp.arange(rows).astype(jnp.float32)[:, None] * THETA ** (-jnp.arange(half, dtype=jnp.float32) / half)
        cos, sin = jnp.cos(angle), jnp.sin(angle)
        cos, sin = jnp.concatenate([cos, cos], 1), jnp.concatenate([-sin, sin], 1)
        order = jnp.stack([1 - core, core]).astype(jnp.int32)
        pairs = range(batch // 2)

        sums = []
        for p in pairs:
            a = norm(x, gain_a, 2 * p, 2)
            v, k, q = matmul(a, wv), matmul(a, wk), matmul(a, wq)
            seen = attention(q, k, v, order, cos, sin, rows)
            sums.append(summed(seen[:rows], seen[rows:], wo, PIECES_A[p]))

        def gated(b):
            up = lax.optimization_barrier(dot(b, w_up))
            return (jax.nn.silu(dot(b, w_gate)) * up).astype(jnp.bfloat16)

        ends = []
        for p in pairs:
            h, both = join(x, gain_m, 2 * p, *sums[p])
            hidden = gated(both)
            here, there = summed(hidden[:rows], hidden[rows:], w_down, PIECES_M[p])
            width = d // len(here)
            ends += [(p, n, width, h[:, n * width : (n + 1) * width], s, t) for n, (s, t) in enumerate(zip(here, there))]

        y, sent = unwritten(x.shape, x.dtype), []

        def put(y, p, n, width, other):
            return lax.dynamic_update_slice(y, other[None], (2 * p + 1 - core, 0, n * width))

        for p, n, width, base, s, t in ends:
            own = joined(base, s, t)
            y = lax.dynamic_update_slice(y, own[None], (2 * p + core, 0, n * width))
            sent.append((p, n, width, lax.ppermute(own, "tp", MATE)))
            if len(sent) > 2:
                y = put(y, *sent.pop(0))
        for late in sent:
            y = put(y, *late)
        return y

    tokens, whole, columns, rows_of = P("dp", None, None), P(None), P(None, "tp"), P("tp", None)
    return jax.shard_map(
        step,
        mesh=mesh,
        in_specs=(tokens, whole, columns, columns, columns, rows_of, whole, columns, columns, rows_of),
        out_specs=tokens,
        check_vma=False,
    )
```
